32 devices in a mesh: batch: 1 (over z), tp: 4 (over y), sp: 8 (over x, core).
Axes of the slice: x: 4, y: 4, z: 1, core: 2. Of those that a mesh axis runs over, the one named last changes fastest.
The devices are a block of a 4x4x8 slice.
Arguments:
- tokens: bfloat16 [16384, 2560], P(('batch', 'sp'))
- glob_pos: int32 [512], P('batch')
- rel_bias: float32 [20, 513], P('tp')
- w_query: bfloat16 [2560, 2560], P(None, 'tp')
- w_key: bfloat16 [2560, 2560], P(None, 'tp')
- w_value: bfloat16 [2560, 2560], P(None, 'tp')
- w_query_glob: bfloat16 [2560, 2560], P(None, 'tp')
- w_out: bfloat16 [2560, 2560], P('tp')
- w_up: bfloat16 [2560, 10240], P(None, 'tp')
- w_down: bfloat16 [10240, 2560], P('tp')
Outputs:
- output: bfloat16 [16384, 2560], P(('batch', 'sp'))
All inputs are finite; a program needn't handle non-finite values.
Results may differ from the reference program's by a relative error of at most 0.0114115.
Values are sent between devices in bfloat16 or wider.
A program may use at most 768 MiB of HBM per device.

```python
import math
import jax
import jax.numpy as jnp
from jax import lax

MODEL_DIM = 2560
NUM_HEADS = 20
HIDDEN_DIM = 10240
WINDOW = 256
NUM_GLOBAL = 512
SEQ_LEN = 16384


def setup_inputs(seed: int = 0, part: int = 0) -> dict:
    part_keys = jax.random.split(jax.random.fold_in(jax.random.key(seed), part), 2)
    shared_keys = jax.random.split(jax.random.key(seed + 1), 9)
    in_scale = MODEL_DIM ** -0.5
    out_scale = ((2 * WINDOW + NUM_GLOBAL) / (3.0 * MODEL_DIM)) ** 0.5
    glob_scale = (math.log(6.0 * SEQ_LEN / (2 * WINDOW + NUM_GLOBAL)) / MODEL_DIM) ** 0.5

    def draw_normal(rand_key, arr_shape, std_dev):
        return (std_dev * jax.random.normal(rand_key, arr_shape, jnp.float32)).astype(jnp.bfloat16)

    square = (MODEL_DIM, MODEL_DIM)
    glob_pos = jnp.sort(jax.random.permutation(part_keys[1], SEQ_LEN)[:NUM_GLOBAL]).astype(jnp.int32)
    return {
        "tokens": draw_normal(part_keys[0], (SEQ_LEN, MODEL_DIM), 1.0),
        "glob_pos": glob_pos,
        "rel_bias": 0.7 * jax.random.normal(shared_keys[0], (NUM_HEADS, 2 * WINDOW + 1), jnp.float32),
        "w_query": draw_normal(shared_keys[1], square, in_scale),
        "w_key": draw_normal(shared_keys[2], square, in_scale),
        "w_value": draw_normal(shared_keys[3], square, in_scale),
        "w_query_glob": draw_normal(shared_keys[4], square, glob_scale),
        "w_out": draw_normal(shared_keys[5], square, out_scale),
        "w_up": draw_normal(shared_keys[6], (MODEL_DIM, HIDDEN_DIM), in_scale),
        "w_down": draw_normal(shared_keys[7], (HIDDEN_DIM, MODEL_DIM), HIDDEN_DIM ** -0.5),
    }


def reference(tokens, glob_pos, rel_bias, w_query, w_key, w_value, w_query_glob, w_out, w_up, w_down):
    head_dim = MODEL_DIM // NUM_HEADS
    score_scale = head_dim ** -0.5
    n_blocks = SEQ_LEN // WINDOW
    heads_shape = (SEQ_LEN, NUM_HEADS, head_dim)

    def project(weight):
        product = jnp.dot(tokens, weight, preferred_element_type=jnp.float32)
        return product.astype(jnp.bfloat16).astype(jnp.float32).reshape(heads_shape)

    queries = project(w_query)
    keys_all = project(w_key)
    values_all = project(w_value)
    zero_pad = jnp.zeros((WINDOW, NUM_HEADS, head_dim), jnp.float32)
    keys_ext = jnp.concatenate([zero_pad, keys_all, zero_pad], axis=0)
    values_ext = jnp.concatenate([zero_pad, values_all, zero_pad], axis=0)
    glob_keys = keys_all[glob_pos]
    glob_values = values_all[glob_pos]
    rel_offs = jnp.arange(3 * WINDOW)[None, :] - jnp.arange(WINDOW)[:, None]
    in_band = (rel_offs >= 0) & (rel_offs <= 2 * WINDOW)
    band_bias = jnp.take(rel_bias, jnp.clip(rel_offs, 0, 2 * WINDOW), axis=1)

    def window_block(blk_index):
        blk_start = blk_index * WINDOW
        q_blk = lax.dynamic_slice_in_dim(queries, blk_start, WINDOW, axis=0)
        k_win = lax.dynamic_slice_in_dim(keys_ext, blk_start, 3 * WINDOW, axis=0)
        v_win = lax.dynamic_slice_in_dim(values_ext, blk_start, 3 * WINDOW, axis=0)
        query_pos = blk_start + jnp.arange(WINDOW)
        key_pos = blk_start - WINDOW + jnp.arange(3 * WINDOW)
        key_ok = (key_pos >= 0) & (key_pos < SEQ_LEN)
        win_scores = jnp.einsum("qhd,khd->hqk", q_blk, k_win) * score_scale + band_bias
        win_scores = jnp.where(in_band & key_ok[None, :], win_scores, -jnp.inf)
        far_mask = jnp.abs(query_pos[:, None] - glob_pos[None, :]) > WINDOW
        glob_scores = jnp.einsum("qhd,ghd->hqg", q_blk, glob_keys) * score_scale
        glob_scores = jnp.where(far_mask, glob_scores, -jnp.inf)
        scores = jnp.concatenate([win_scores, glob_scores], axis=-1)
        attn_probs = jax.nn.softmax(scores, axis=-1).astype(jnp.bfloat16).astype(jnp.float32)
        all_values = jnp.concatenate([v_win, glob_values], axis=0)
        return jnp.einsum("hqk,khd->qhd", attn_probs, all_values)

    win_out = lax.map(window_block, jnp.arange(n_blocks)).reshape(heads_shape)
    x_glob = tokens[glob_pos]
    q_glob = jnp.dot(x_glob, w_query_glob, preferred_element_type=jnp.float32)
    q_glob = q_glob.astype(jnp.bfloat16).astype(jnp.float32).reshape(NUM_GLOBAL // 8, 8, NUM_HEADS, head_dim)

    def glob_block(q_group):
        scores = jnp.einsum("ghd,khd->hgk", q_group, keys_all) * score_scale
        attn_probs = jax.nn.softmax(scores, axis=-1).astype(jnp.bfloat16).astype(jnp.float32)
        return jnp.einsum("hgk,khd->ghd", attn_probs, values_all)

    glob_out = lax.map(glob_block, q_glob).reshape(NUM_GLOBAL, NUM_HEADS, head_dim)
    heads_out = win_out.at[glob_pos].set(glob_out)
    attn_vec = heads_out.reshape(SEQ_LEN, MODEL_DIM).astype(jnp.bfloat16)
    attn_proj = jnp.dot(attn_vec, w_out, preferred_element_type=jnp.float32)
    hidden = (tokens.astype(jnp.float32) + attn_proj).astype(jnp.bfloat16)
    up_proj = jnp.dot(hidden, w_up, preferred_element_type=jnp.float32)
    act_vals = jax.nn.gelu(up_proj).astype(jnp.bfloat16)
    down_proj = jnp.dot(act_vals, w_down, preferred_element_type=jnp.float32)
    return (hidden.astype(jnp.float32) + down_proj).astype(jnp.bfloat16)
```

```python
import functools
import math

import jax
import jax.numpy as jnp
from jax import lax
from jax.experimental import pallas as pl
from jax.experimental.pallas import tpu as pltpu
from jax.sharding import PartitionSpec as P

LOG2E = math.log2(math.e)
NEG_INF = float("-inf")
F32 = jnp.float32
BF16 = jnp.bfloat16


def _dot(lhs, rhs):
    return jnp.dot(lhs, rhs, preferred_element_type=F32)


def _dot_t(lhs, rhs):
    return lax.dot_general(lhs, rhs, (((1,), (1,)), ((), ())), preferred_element_type=F32)


def _qkv_kernel(x_ref, wq_ref, wk_ref, wv_ref, q_ref, k_ref, v_ref):
    x = x_ref[...]
    q_ref[...] = _dot(x, wq_ref[...]).astype(BF16)
    k_ref[...] = _dot(x, wk_ref[...]).astype(BF16)
    v_ref[...] = _dot(x, wv_ref[...]).astype(BF16)


def _project_qkv(tokens, w_query, w_key, w_value):
    rows, depth = tokens.shape
    cols = w_query.shape[1]
    blk = rows // 4
    w_spec = pl.BlockSpec((depth, cols), lambda i: (0, 0), pipeline_mode=pl.Buffered(1))
    o_spec = pl.BlockSpec((blk, cols), lambda i: (i, 0))
    return pl.pallas_call(
        _qkv_kernel,
        grid=(rows // blk,),
        in_specs=[pl.BlockSpec((blk, depth), lambda i: (i, 0)), w_spec, w_spec, w_spec],
        out_specs=[o_spec] * 3,
        out_shape=[jax.ShapeDtypeStruct((rows, cols), BF16)] * 3,
        cost_estimate=pl.CostEstimate(
            flops=6 * rows * depth * cols,
            bytes_accessed=2 * (rows * depth + 3 * depth * cols + 3 * rows * cols),
            transcendentals=0,
        ),
        name="qkv_proj",
    )(tokens, w_query, w_key, w_value)


def _glob_kernel(scale, q_ref, k_ref, v_ref, o_ref, m_ref, l_ref):
    scores = _dot_t(q_ref[...], k_ref[...]) * scale
    top = jnp.max(scores, axis=1, keepdims=True)
    probs = jnp.exp2(scores - top)
    total = jnp.sum(probs, axis=1, keepdims=True)
    o_ref[...] = _dot(probs.astype(BF16), v_ref[...])
    m_ref[...] = jnp.broadcast_to(top, m_ref.shape)
    l_ref[...] = jnp.broadcast_to(total, l_ref.shape)


def _glob_partial(glob_q, keys, values, n_heads, scale):
    n_glob, width = glob_q.shape
    rows = keys.shape[0]
    hd = width // n_heads
    blk = n_glob // 2
    q_spec = pl.BlockSpec((blk, hd), lambda h, i: (i, h))
    kv_spec = pl.BlockSpec((rows, hd), lambda h, i: (0, h))
    return pl.pallas_call(
        functools.partial(_glob_kernel, scale * LOG2E),
        grid=(n_heads, n_glob // blk),
        in_specs=[q_spec, kv_spec, kv_spec],
        out_specs=[q_spec] * 3,
        out_shape=[jax.ShapeDtypeStruct((n_glob, width), F32)] * 3,
        cost_estimate=pl.CostEstimate(
            flops=16 * n_glob * rows * width,
            bytes_accessed=4 * rows * width + 14 * n_glob * width,
            transcendentals=n_glob * rows * n_heads,
        ),
        name="glob_attn",
    )(glob_q, keys, values)


def _local_kernel(window, seq_len, scale, start_ref, q_ref, k_ref, v_ref, gk_ref, gv_ref, rb_ref, gpos_ref, o_ref, bias_ref):
    blk = pl.program_id(1)
    span = 3 * window

    @pl.when(blk == 0)
    def _():
        bias = jnp.broadcast_to(rb_ref[0], (window, span))
        row = lax.broadcasted_iota(jnp.int32, (window, span), 0)
        for bit in range(window.bit_length() - 1):
            bias = jnp.where(((row >> bit) & 1) == 1, pltpu.roll(bias, 1 << bit, 1), bias)
        bias_ref[...] = bias

    first = start_ref[0] + blk * window
    key_pos = first - window + lax.broadcasted_iota(jnp.int32, (1, span), 1)
    edge = jnp.where((key_pos >= 0) & (key_pos < seq_len), 0.0, NEG_INF).astype(F32)
    q = q_ref[...]
    rows = pl.ds(pl.multiple_of(blk * window, window), span)
    win = _dot_t(q, k_ref[rows, :]) * scale + (bias_ref[...] + edge)
    dist = first + lax.broadcasted_iota(jnp.int32, (window, 1), 0) - gpos_ref[...]
    glob = _dot_t(q, gk_ref[...]) * scale
    glob = jnp.where(jnp.abs(dist) > window, glob, NEG_INF)
    top = jnp.maximum(jnp.max(win, axis=1, keepdims=True), jnp.max(glob, axis=1, keepdims=True))
    win = jnp.exp2(win - top)
    glob = jnp.exp2(glob - top)
    inv = 1.0 / (jnp.sum(win, axis=1, keepdims=True) + jnp.sum(glob, axis=1, keepdims=True))
    out = _dot((win * inv).astype(BF16), v_ref[rows, :])
    out = out + _dot((glob * inv).astype(BF16), gv_ref[...])
    o_ref[...] = out.astype(BF16)


def _local_attn(row_start, q, k_ext, v_ext, glob_k, glob_v, rel_bias, glob_pos, window, seq_len, scale):
    rows, width = q.shape
    n_heads = rel_bias.shape[0]
    hd = width // n_heads
    n_glob = glob_k.shape[0]
    span = 3 * window
    pad = jnp.full((n_heads, span - rel_bias.shape[1]), NEG_INF, F32)
    bias_rows = jnp.concatenate([rel_bias * LOG2E, pad], axis=1)[:, None, :]
    q_spec = pl.BlockSpec((window, hd), lambda h, c, s: (c, h))
    kv_spec = pl.BlockSpec((k_ext.shape[0], hd), lambda h, c, s: (0, h))
    g_spec = pl.BlockSpec((n_glob, hd), lambda h, c, s: (0, h))
    grid_spec = pltpu.PrefetchScalarGridSpec(
        num_scalar_prefetch=1,
        grid=(n_heads, rows // window),
        in_specs=[
            q_spec,
            kv_spec,
            kv_spec,
            g_spec,
            g_spec,
            pl.BlockSpec((1, 1, span), lambda h, c, s: (h, 0, 0)),
            pl.BlockSpec((1, n_glob), lambda h, c, s: (0, 0)),
        ],
        out_specs=q_spec,
        scratch_shapes=[pltpu.VMEM((window, span), F32)],
    )
    return pl.pallas_call(
        functools.partial(_local_kernel, window, seq_len, scale * LOG2E),
        grid_spec=grid_spec,
        out_shape=jax.ShapeDtypeStruct((rows, width), BF16),
        cost_estimate=pl.CostEstimate(
            flops=16 * rows * (span + n_glob) * width,
            bytes_accessed=2 * (2 * rows * width + 2 * (k_ext.shape[0] + n_glob) * width),
            transcendentals=n_heads * rows * (span + n_glob),
        ),
        name="local_attn",
    )(row_start[None], q, k_ext, v_ext, glob_k, glob_v, bias_rows, glob_pos[None, :])


def solution(mesh):
    n_seq = mesh.shape["sp"]
    n_tp = mesh.shape["tp"]
    to_right = [(sender, sender + 1) for sender in range(n_seq - 1)]
    to_left = [(sender + 1, sender) for sender in range(n_seq - 1)]
    n_row_chunks = 2
    n_hid_chunks = 2

    def local_layer(tokens, glob_pos, rel_bias, w_query, w_key, w_value, w_query_glob, w_out, w_up, w_down):
        local_rows, model_dim = tokens.shape
        n_heads, rel_width = rel_bias.shape
        window = (rel_width - 1) // 2
        width = w_query.shape[1]
        hd = width // n_heads
        n_glob = glob_pos.shape[0]
        seq_len = local_rows * n_seq
        scale = hd ** -0.5
        sp_index = lax.axis_index("sp")
        tp_index = lax.axis_index("tp")
        row_start = (sp_index * local_rows).astype(jnp.int32)

        def share(shard):
            part = shard.shape[0] // n_seq
            piece = lax.dynamic_slice_in_dim(shard, sp_index * part, part, 0)
            return lax.all_gather(piece, ("tp", "sp"), axis=0, tiled=True)

        hid = w_up.shape[1] // n_hid_chunks
        out_full = share(w_out)
        up_full, down_full = [], []
        for j in range(n_hid_chunks):
            up_full.append(share(w_up[:, j * hid:(j + 1) * hid]).reshape(n_tp, model_dim, hid))
            down_full.append(share(w_down[j * hid:(j + 1) * hid]))

        q, k, v = _project_qkv(tokens, w_query, w_key, w_value)

        edges = jnp.stack([k, v])
        left = lax.ppermute(edges[:, local_rows - window:], "sp", to_right)
        right = lax.ppermute(edges[:, :window], "sp", to_left)
        k_ext = jnp.concatenate([left[0], k, right[0]], axis=0)
        v_ext = jnp.concatenate([left[1], v, right[1]], axis=0)

        slot = glob_pos - row_start
        pick = (slot[:, None] == jnp.arange(local_rows, dtype=jnp.int32)[None, :]).astype(BF16)
        qg_rows = _dot(_dot(pick, tokens).astype(BF16), w_query_glob).astype(BF16)
        mine = jnp.concatenate([qg_rows, _dot(pick, k).astype(BF16), _dot(pick, v).astype(BF16)], axis=1)
        mine = lax.all_to_all(mine, "sp", 0, 0, tiled=True)
        mine = mine.reshape(n_seq, n_glob // n_seq, 3 * width)
        mine = mine.astype(F32).sum(axis=0).astype(BF16)
        glob_q = lax.all_gather(mine[:, :width], "sp", axis=0, tiled=True)
        glob_k = lax.all_gather(mine[:, width:2 * width], "sp", axis=0, tiled=True)
        glob_v = lax.all_gather(mine[:, 2 * width:], "sp", axis=0, tiled=True)

        part_out, part_max, part_sum = _glob_partial(glob_q, k, v, n_heads, scale)
        parts = jnp.concatenate([part_out, part_max[:, ::hd], part_sum[:, ::hd]], axis=1)
        parts = lax.all_to_all(parts, "sp", 0, 0, tiled=True)
        parts = parts.reshape(n_seq, n_glob // n_seq, width + 2 * n_heads)
        part_max = parts[:, :, width:width + n_heads]
        factor = jnp.exp2(part_max - part_max.max(axis=0))
        tot_sum = (parts[:, :, width + n_heads:] * factor).sum(axis=0)
        part_out = parts[:, :, :width].reshape(n_seq, n_glob // n_seq, n_heads, hd)
        tot_out = (part_out * factor[..., None]).sum(axis=0) / tot_sum[..., None]
        glob_out = tot_out.astype(BF16).reshape(n_glob // n_seq, width)
        glob_out = lax.all_gather(glob_out, "sp", axis=0, tiled=True)

        win_out = _local_attn(row_start, q, k_ext, v_ext, glob_k, glob_v, rel_bias, glob_pos, window, seq_len, scale)

        put = jnp.arange(local_rows, dtype=jnp.int32)[:, None] == slot[None, :]
        is_glob = put.any(axis=1, keepdims=True)
        heads_out = jnp.where(is_glob, _dot(put.astype(BF16), glob_out).astype(BF16), win_out)

        blk = local_rows // (n_row_chunks * n_tp)
        heads_out = heads_out.reshape(n_row_chunks, n_tp, blk, width)
        heads_out = lax.all_to_all(heads_out, "tp", 1, 1, tiled=True)
        attn_rows = heads_out.transpose(0, 2, 1, 3).reshape(n_row_chunks * blk, n_tp * width)
        own_rows = lax.dynamic_index_in_dim(tokens.reshape(n_row_chunks, n_tp, blk, model_dim), tp_index, 1, keepdims=False)
        own_rows = own_rows.reshape(n_row_chunks * blk, model_dim)
        hidden = (own_rows.astype(F32) + _dot(attn_rows, out_full)).astype(BF16)

        acts = [
            jnp.concatenate([jax.nn.gelu(_dot(hidden, w)).astype(BF16) for w in up_full[j]], axis=1)
            for j in range(n_hid_chunks)
        ]
        acc = sum(_dot(acts[j], down_full[j]) for j in range(n_hid_chunks - 1))
        outs = []
        for i in range(n_row_chunks):
            rows = slice(i * blk, (i + 1) * blk)
            mlp = acc[rows] + _dot(acts[-1][rows], down_full[-1])
            out = (hidden[rows].astype(F32) + mlp).astype(BF16)
            outs.append(lax.all_gather(out, "tp", axis=0, tiled=True))
        return jnp.concatenate(outs, axis=0)

    row_spec = P(("batch", "sp"), None)
    col_spec = P(None, "tp")
    head_spec = P("tp", None)
    in_specs = (row_spec, P("batch"), head_spec, col_spec, col_spec, col_spec, col_spec, head_spec, col_spec, head_spec)
    return jax.shard_map(local_layer, mesh=mesh, in_specs=in_specs, out_specs=row_spec, check_vma=False)
```

```python
import functools
import math

import jax
import jax.numpy as jnp
from jax import lax
from jax.experimental import pallas as pl
from jax.experimental.pallas import tpu as pltpu
from jax.sharding import PartitionSpec as P


LOG2E = math.log2(math.e)
NEG_INF = float("-inf")
F32 = jnp.float32
BF16 = jnp.bfloat16


def _dot(lhs, rhs):
    return jnp.dot(lhs, rhs, preferred_element_type=F32)


def _dot_t(lhs, rhs):
    return lax.dot_general(lhs, rhs, (((1,), (1,)), ((), ())), preferred_element_type=F32)


def _proj_kernel(x_ref, *refs):
    x = x_ref[...]
    n_out = len(refs) // 2
    for w_ref, o_ref in zip(refs[:n_out], refs[n_out:]):
        o_ref[...] = _dot(x, w_ref[...]).astype(BF16)


def _project(tokens, *weights):
    rows, depth = tokens.shape
    cols = weights[0].shape[1]
    n_out = len(weights)
    blk = rows // 4
    w_spec = pl.BlockSpec((depth, cols), lambda i: (0, 0), pipeline_mode=pl.Buffered(1))
    o_spec = pl.BlockSpec((blk, cols), lambda i: (i, 0))
    return pl.pallas_call(
        _proj_kernel,
        grid=(rows // blk,),
        in_specs=[pl.BlockSpec((blk, depth), lambda i: (i, 0))] + [w_spec] * n_out,
        out_specs=[o_spec] * n_out,
        out_shape=[jax.ShapeDtypeStruct((rows, cols), BF16)] * n_out,
        cost_estimate=pl.CostEstimate(
            flops=2 * n_out * rows * depth * cols,
            bytes_accessed=2 * (rows * depth + n_out * depth * cols + n_out * rows * cols),
            transcendentals=0,
        ),
    )(tokens, *weights)


def _glob_kernel(scale, n_heads, q_ref, k_ref, v_ref, o_ref):
    hd = q_ref.shape[1] // n_heads
    rows, lanes = q_ref.shape[0], o_ref.shape[1] - q_ref.shape[1]
    lane = lax.broadcasted_iota(jnp.int32, (rows, lanes), 1)
    stats = jnp.zeros((rows, lanes), F32)
    for h in range(n_heads):
        cols = slice(h * hd, (h + 1) * hd)
        scores = _dot_t(q_ref[:, cols], k_ref[:, cols]) * scale
        top = jnp.max(scores, axis=1, keepdims=True)
        probs = jnp.exp2(scores - top)
        total = jnp.sum(probs, axis=1, keepdims=True)
        o_ref[:, cols] = _dot(probs.astype(BF16), v_ref[:, cols])
        stats = jnp.where(lane == h, top, jnp.where(lane == n_heads + h, total, stats))
    o_ref[:, q_ref.shape[1]:] = stats


def _glob_partial(glob_q, keys, values, n_heads, scale):
    n_glob, width = glob_q.shape
    rows = keys.shape[0]
    blk = n_glob // 4
    out_width = width + 128
    kv_spec = pl.BlockSpec((rows, width), lambda i: (0, 0), pipeline_mode=pl.Buffered(1))
    return pl.pallas_call(
        functools.partial(_glob_kernel, scale * LOG2E, n_heads),
        grid=(n_glob // blk,),
        in_specs=[pl.BlockSpec((blk, width), lambda i: (i, 0)), kv_spec, kv_spec],
        out_specs=pl.BlockSpec((blk, out_width), lambda i: (i, 0)),
        out_shape=jax.ShapeDtypeStruct((n_glob, out_width), F32),
        cost_estimate=pl.CostEstimate(
            flops=16 * n_glob * rows * width,
            bytes_accessed=4 * rows * width + 6 * n_glob * width,
            transcendentals=n_glob * rows * n_heads,
        ),
        name="glob_attn",
    )(glob_q, keys, values)


def _local_kernel(
    window, seq_len, scale, n_heads, start_ref, q_ref, k_ref, v_ref, kl_ref, kr_ref, vl_ref, vr_ref,
    gk_ref, gv_ref, rb_ref, gpos_ref, o_ref, k_ext, v_ext, bias_ref,
):
    blk = pl.program_id(0)
    span = 3 * window
    rows_all = k_ref.shape[0]
    hd = q_ref.shape[1] // n_heads

    @pl.when(blk == 0)
    def _():
        for ext, left, mid, right in ((k_ext, kl_ref, k_ref, kr_ref), (v_ext, vl_ref, v_ref, vr_ref)):
            ext[:window] = left[...]
            ext[window:window + rows_all] = mid[...]
            ext[window + rows_all:] = right[...]
        row = lax.broadcasted_iota(jnp.int32, (window, span), 0)
        for h in range(n_heads):
            bias = jnp.broadcast_to(rb_ref[h], (window, span))
            for bit in range(window.bit_length() - 1):
                bias = jnp.where(((row >> bit) & 1) == 1, pltpu.roll(bias, 1 << bit, 1), bias)
            bias_ref[h] = bias

    first = start_ref[0] + blk * window
    key_pos = first - window + lax.broadcasted_iota(jnp.int32, (1, span), 1)
    edge = jnp.where((key_pos >= 0) & (key_pos < seq_len), 0.0, NEG_INF).astype(F32)
    dist = first + lax.broadcasted_iota(jnp.int32, (window, 1), 0) - gpos_ref[...]
    far = jnp.where(jnp.abs(dist) > window, 0.0, NEG_INF).astype(F32)
    rows = pl.ds(pl.multiple_of(blk * window, window), span)
    for h in range(n_heads):
        cols = slice(h * hd, (h + 1) * hd)
        q = q_ref[:, cols]
        win = _dot_t(q, k_ext[rows, cols]) * scale + (bias_ref[h] + edge)
        glob = _dot_t(q, gk_ref[:, cols]) * scale + far
        top = jnp.maximum(jnp.max(win, axis=1, keepdims=True), jnp.max(glob, axis=1, keepdims=True))
        win = jnp.exp2(win - top)
        glob = jnp.exp2(glob - top)
        inv = 1.0 / (jnp.sum(win, axis=1, keepdims=True) + jnp.sum(glob, axis=1, keepdims=True))
        out = _dot((win * inv).astype(BF16), v_ext[rows, cols])
        out = out + _dot((glob * inv).astype(BF16), gv_ref[:, cols])
        o_ref[:, cols] = out.astype(BF16)


def _local_attn(row_start, q, k, v, k_left, k_right, v_left, v_right, glob_k, glob_v, rel_bias, glob_pos, window, seq_len, scale):
    rows, width = q.shape
    n_heads = rel_bias.shape[0]
    n_glob = glob_k.shape[0]
    span = 3 * window
    pad = jnp.full((n_heads, span - rel_bias.shape[1]), NEG_INF, F32)
    bias_rows = jnp.concatenate([rel_bias * LOG2E, pad], axis=1)[:, None, :]

    def whole(array):
        return pl.BlockSpec(array.shape, lambda c, s: (0,) * array.ndim, pipeline_mode=pl.Buffered(1))

    q_spec = pl.BlockSpec((window, width), lambda c, s: (c, 0))
    held = (k, v, k_left, k_right, v_left, v_right, glob_k, glob_v, bias_rows, glob_pos[None, :])
    grid_spec = pltpu.PrefetchScalarGridSpec(
        num_scalar_prefetch=1,
        grid=(rows // window,),
        in_specs=[q_spec] + [whole(array) for array in held],
        out_specs=q_spec,
        scratch_shapes=[
            pltpu.VMEM((rows + 2 * window, width), BF16),
            pltpu.VMEM((rows + 2 * window, width), BF16),
            pltpu.VMEM((n_heads, window, span), F32),
        ],
    )
    return pl.pallas_call(
        functools.partial(_local_kernel, window, seq_len, scale * LOG2E, n_heads),
        grid_spec=grid_spec,
        out_shape=jax.ShapeDtypeStruct((rows, width), BF16),
        cost_estimate=pl.CostEstimate(
            flops=16 * rows * (span + n_glob) * width,
            bytes_accessed=2 * (2 * rows * width + 2 * (rows + 2 * window + n_glob) * width),
            transcendentals=n_heads * rows * (span + n_glob),
        ),
        name="local_attn",
    )(row_start[None], q, *held)


def solution(mesh):
    n_seq = mesh.shape["sp"]
    n_tp = mesh.shape["tp"]
    to_right = [(sender, sender + 1) for sender in range(n_seq - 1)]
    to_left = [(sender + 1, sender) for sender in range(n_seq - 1)]
    to_next = [(sender, (sender + 1) % n_tp) for sender in range(n_tp)]
    to_prev = [(sender, (sender - 1) % n_tp) for sender in range(n_tp)]
    to_twin = [(sender, (sender + n_tp // 2) % n_tp) for sender in range(n_tp)]
    assert n_tp == 4

    def layer(tokens, glob_pos, rel_bias, w_query, w_key, w_value, w_query_glob, w_out, w_up, w_down):
        local_rows, model_dim = tokens.shape
        n_heads, rel_width = rel_bias.shape
        window = (rel_width - 1) // 2
        width = w_query.shape[1]
        hd = width // n_heads
        n_glob = glob_pos.shape[0]
        glob_blk = n_glob // n_seq
        seq_len = local_rows * n_seq
        scale = hd ** -0.5
        sp_index = lax.axis_index("sp")
        tp_index = lax.axis_index("tp")
        row_start = (sp_index * local_rows).astype(jnp.int32)

        def piece(shard):
            part = shard.shape[0] // n_seq
            return lax.dynamic_slice_in_dim(shard, sp_index * part, part, 0)

        out_full = lax.all_gather(piece(w_out), ("tp", "sp"), axis=0, tiled=True)
        up_piece = lax.ppermute(piece(w_up), "tp", to_twin)
        down_piece = lax.ppermute(piece(w_down), "tp", to_twin)
        up_twin = lax.all_gather(up_piece, "sp", axis=0, tiled=True)
        down_twin = lax.all_gather(down_piece, "sp", axis=0, tiled=True)

        slot = glob_pos - row_start
        pick = (slot[:, None] == jnp.arange(local_rows, dtype=jnp.int32)[None, :]).astype(BF16)
        glob_rows = _dot(pick, tokens).astype(BF16)
        glob_rows = lax.all_to_all(glob_rows, "sp", 0, 0, tiled=True)

        k, v = _project(tokens, w_key, w_value)
        (q,) = _project(tokens, w_query)
        k_left = lax.ppermute(k[local_rows - window:], "sp", to_right)
        v_left = lax.ppermute(v[local_rows - window:], "sp", to_right)
        k_right = lax.ppermute(k[:window], "sp", to_left)
        v_right = lax.ppermute(v[:window], "sp", to_left)

        def to_all(block):
            copies = jnp.broadcast_to(block[None], (n_seq,) + block.shape)
            return lax.all_to_all(copies, "sp", 0, 0, tiled=True).reshape(n_seq * block.shape[0], block.shape[1])

        glob_rows = glob_rows.reshape(n_seq, glob_blk, model_dim).astype(F32).sum(axis=0).astype(BF16)
        glob_qkv = jnp.concatenate([_dot(glob_rows, w).astype(BF16) for w in (w_query_glob, w_key, w_value)], axis=1)
        glob_qkv = to_all(glob_qkv)
        glob_q = glob_qkv[:, :width]
        glob_k = glob_qkv[:, width:2 * width]
        glob_v = glob_qkv[:, 2 * width:]

        parts = _glob_partial(glob_q, k, v, n_heads, scale)
        parts = lax.all_to_all(parts, "sp", 0, 0, tiled=True).reshape(n_seq, glob_blk, parts.shape[1])
        part_max = parts[:, :, width:width + n_heads]
        factor = jnp.exp2(part_max - part_max.max(axis=0))
        tot_sum = (parts[:, :, width + n_heads:width + 2 * n_heads] * factor).sum(axis=0)
        part_out = parts[:, :, :width].reshape(n_seq, glob_blk, n_heads, hd)
        tot_out = (part_out * factor[..., None]).sum(axis=0) / tot_sum[..., None]
        glob_out = to_all(tot_out.astype(BF16).reshape(glob_blk, width))

        win_out = _local_attn(
            row_start, q, k, v, k_left, k_right, v_left, v_right, glob_k, glob_v, rel_bias, glob_pos, window, seq_len, scale
        )

        put = jnp.arange(local_rows, dtype=jnp.int32)[:, None] == slot[None, :]
        is_glob = put.any(axis=1, keepdims=True)
        heads_out = jnp.where(is_glob, _dot(put.astype(BF16), glob_out).astype(BF16), win_out)

        blk = local_rows // (2 * n_tp)
        heads_out = heads_out.reshape(2, n_tp, blk, width)
        heads_out = lax.all_to_all(heads_out, "tp", 1, 1, tiled=True)
        attn_rows = heads_out.transpose(0, 2, 1, 3).reshape(2 * blk, n_tp * width)
        own_rows = lax.dynamic_index_in_dim(tokens.reshape(2, n_tp, blk, model_dim), tp_index, 1, keepdims=False)
        own_rows = own_rows.reshape(2 * blk, model_dim)
        hidden = (own_rows.astype(F32) + _dot(attn_rows, out_full)).astype(BF16)

        def act(rows, weight):
            return jax.nn.gelu(_dot(rows, weight)).astype(BF16)

        from_prev = lax.ppermute(hidden[:blk], "tp", to_next)
        from_next = lax.ppermute(hidden[blk:], "tp", to_prev)
        own_act, own_act_twin = act(hidden, w_up), act(hidden, up_twin)
        guests = jnp.concatenate([from_prev, from_next], axis=0)
        guest_part = _dot(act(guests, w_up), w_down) + _dot(act(guests, up_twin), down_twin)
        back_first = lax.ppermute(guest_part[:blk], "tp", to_prev)
        back_second = lax.ppermute(guest_part[blk:], "tp", to_next)
        own_part = _dot(own_act, w_down) + _dot(own_act_twin, down_twin)
        outs = []
        for rows, back in ((slice(0, blk), back_first), (slice(blk, 2 * blk), back_second)):
            out = (hidden[rows].astype(F32) + (own_part[rows] + back)).astype(BF16)
            outs.append(lax.all_gather(out, "tp", axis=0, tiled=True))
        return jnp.concatenate(outs, axis=0)

    row_spec = P(("batch", "sp"), None)
    col_spec = P(None, "tp")
    head_spec = P("tp", None)
    in_specs = (row_spec, P("batch"), head_spec, col_spec, col_spec, col_spec, col_spec, head_spec, col_spec, head_spec)
    return jax.shard_map(layer, mesh=mesh, in_specs=in_specs, out_specs=row_spec, check_vma=False)
```

```python
import functools
import math

import jax
import jax.numpy as jnp
from jax import lax
from jax.experimental import pallas as pl
from jax.experimental.pallas import tpu as pltpu
from jax.sharding import PartitionSpec as P


LOG2E = math.log2(math.e)
NEG_INF = float("-inf")
F32 = jnp.float32
BF16 = jnp.bfloat16


def _dot(lhs, rhs):
    return jnp.dot(lhs, rhs, preferred_element_type=F32)


def _dot_t(lhs, rhs):
    return lax.dot_general(lhs, rhs, (((1,), (1,)), ((), ())), preferred_element_type=F32)


def _proj_kernel(x_ref, *refs):
    x = x_ref[...]
    n_out = len(refs) // 2
    for w_ref, o_ref in zip(refs[:n_out], refs[n_out:]):
        o_ref[...] = _dot(x, w_ref[...]).astype(BF16)


def _project(tokens, *weights):
    rows, depth = tokens.shape
    cols = weights[0].shape[1]
    n_out = len(weights)
    blk = rows // 4
    w_spec = pl.BlockSpec((depth, cols), lambda i: (0, 0), pipeline_mode=pl.Buffered(1))
    o_spec = pl.BlockSpec((blk, cols), lambda i: (i, 0))
    return pl.pallas_call(
        _proj_kernel,
        grid=(rows // blk,),
        in_specs=[pl.BlockSpec((blk, depth), lambda i: (i, 0))] + [w_spec] * n_out,
        out_specs=[o_spec] * n_out,
        out_shape=[jax.ShapeDtypeStruct((rows, cols), BF16)] * n_out,
        cost_estimate=pl.CostEstimate(
            flops=2 * n_out * rows * depth * cols,
            bytes_accessed=2 * (rows * depth + n_out * depth * cols + n_out * rows * cols),
            transcendentals=0,
        ),
    )(tokens, *weights)


def _glob_kernel(scale, n_heads, q_ref, k_ref, v_ref, o_ref):
    hd = q_ref.shape[1] // n_heads
    rows, lanes = q_ref.shape[0], o_ref.shape[1] - q_ref.shape[1]
    lane = lax.broadcasted_iota(jnp.int32, (rows, lanes), 1)
    stats = jnp.zeros((rows, lanes), F32)
    for h in range(n_heads):
        cols = slice(h * hd, (h + 1) * hd)
        scores = _dot_t(q_ref[:, cols], k_ref[:, cols]) * scale
        top = jnp.max(scores, axis=1, keepdims=True)
        probs = jnp.exp2(scores - top)
        total = jnp.sum(probs, axis=1, keepdims=True)
        o_ref[:, cols] = _dot(probs.astype(BF16), v_ref[:, cols])
        stats = jnp.where(lane == h, top, jnp.where(lane == n_heads + h, total, stats))
    o_ref[:, q_ref.shape[1]:] = stats


def _glob_partial(glob_q, keys, values, n_heads, scale):
    n_glob, width = glob_q.shape
    rows = keys.shape[0]
    blk = n_glob // 4
    out_width = width + 128
    kv_spec = pl.BlockSpec((rows, width), lambda i: (0, 0), pipeline_mode=pl.Buffered(1))
    return pl.pallas_call(
        functools.partial(_glob_kernel, scale * LOG2E, n_heads),
        grid=(n_glob // blk,),
        in_specs=[pl.BlockSpec((blk, width), lambda i: (i, 0)), kv_spec, kv_spec],
        out_specs=pl.BlockSpec((blk, out_width), lambda i: (i, 0)),
        out_shape=jax.ShapeDtypeStruct((n_glob, out_width), F32),
        cost_estimate=pl.CostEstimate(
            flops=16 * n_glob * rows * width,
            bytes_accessed=4 * rows * width + 6 * n_glob * width,
            transcendentals=n_glob * rows * n_heads,
        ),
        name="glob_attn",
    )(glob_q, keys, values)


def _local_kernel(
    half, window, seq_len, scale, n_heads, start_ref, q_ref, k_ref, v_ref, kh_ref, vh_ref,
    gk_ref, gv_ref, rb_ref, gpos_ref, o_ref, k_ext, v_ext, bias_ref,
):
    blk = pl.program_id(0)
    span = 3 * window
    rows_all = k_ref.shape[0]
    held = k_ext.shape[0] - window
    hd = q_ref.shape[1] // n_heads

    @pl.when(blk == 0)
    def _():
        for ext, mid, halo in ((k_ext, k_ref, kh_ref), (v_ext, v_ref, vh_ref)):
            if half == 0:
                ext[:window] = halo[...]
                ext[window:] = mid[:held]
            else:
                ext[:held] = mid[rows_all - held:]
                ext[held:] = halo[...]
        row = lax.broadcasted_iota(jnp.int32, (window, span), 0)
        for h in range(n_heads):
            bias = jnp.broadcast_to(rb_ref[h], (window, span))
            for bit in range(window.bit_length() - 1):
                bias = jnp.where(((row >> bit) & 1) == 1, pltpu.roll(bias, 1 << bit, 1), bias)
            bias_ref[h] = bias

    first = start_ref[0] + half * (rows_all // 2) + blk * window
    key_pos = first - window + lax.broadcasted_iota(jnp.int32, (1, span), 1)
    edge = jnp.where((key_pos >= 0) & (key_pos < seq_len), 0.0, NEG_INF).astype(F32)
    dist = first + lax.broadcasted_iota(jnp.int32, (window, 1), 0) - gpos_ref[...]
    far = jnp.where(jnp.abs(dist) > window, 0.0, NEG_INF).astype(F32)
    rows = pl.ds(pl.multiple_of(blk * window, window), span)
    for h in range(n_heads):
        cols = slice(h * hd, (h + 1) * hd)
        q = q_ref[:, cols]
        win = _dot_t(q, k_ext[rows, cols]) * scale + (bias_ref[h] + edge)
        glob = _dot_t(q, gk_ref[:, cols]) * scale + far
        top = jnp.maximum(jnp.max(win, axis=1, keepdims=True), jnp.max(glob, axis=1, keepdims=True))
        win = jnp.exp2(win - top)
        glob = jnp.exp2(glob - top)
        inv = 1.0 / (jnp.sum(win, axis=1, keepdims=True) + jnp.sum(glob, axis=1, keepdims=True))
        out = _dot((win * inv).astype(BF16), v_ext[rows, cols])
        out = out + _dot((glob * inv).astype(BF16), gv_ref[:, cols])
        o_ref[:, cols] = out.astype(BF16)


def _local_attn(half, row_start, q, k, v, k_halo, v_halo, glob_k, glob_v, bias_rows, glob_pos, window, seq_len, scale):
    rows, width = q.shape[0] // 2, q.shape[1]
    n_heads = bias_rows.shape[0]
    n_glob = glob_k.shape[0]
    span = 3 * window
    n_blk = rows // window

    def whole(array):
        return pl.BlockSpec(array.shape, lambda c, s: (0,) * array.ndim, pipeline_mode=pl.Buffered(1))

    held = (k, v, k_halo, v_halo, glob_k, glob_v, bias_rows, glob_pos[None, :])
    grid_spec = pltpu.PrefetchScalarGridSpec(
        num_scalar_prefetch=1,
        grid=(n_blk,),
        in_specs=[pl.BlockSpec((window, width), lambda c, s: (c + half * n_blk, 0))] + [whole(array) for array in held],
        out_specs=pl.BlockSpec((window, width), lambda c, s: (c, 0)),
        scratch_shapes=[
            pltpu.VMEM((rows + 2 * window, width), BF16),
            pltpu.VMEM((rows + 2 * window, width), BF16),
            pltpu.VMEM((n_heads, window, span), F32),
        ],
    )
    return pl.pallas_call(
        functools.partial(_local_kernel, half, window, seq_len, scale * LOG2E, n_heads),
        grid_spec=grid_spec,
        out_shape=jax.ShapeDtypeStruct((rows, width), BF16),
        cost_estimate=pl.CostEstimate(
            flops=16 * rows * (span + n_glob) * width,
            bytes_accessed=2 * (2 * rows * width + 2 * (rows + 2 * window + n_glob) * width),
            transcendentals=n_heads * rows * (span + n_glob),
        ),
    )(row_start[None], q, *held)


def _mlp_kernel(n_steps, x_ref, up_ref, down_ref, *refs):
    o_ref, act_ref = refs[-2:]
    step = pl.program_id(0)

    def rise():
        return jax.nn.gelu(_dot(x_ref[...], up_ref[...])).astype(BF16)

    @pl.when(step == 0)
    def _():
        act_ref[...] = rise()
        o_ref[...] = refs[0][...] if len(refs) == 3 else jnp.zeros_like(o_ref)

    @pl.when((step > 0) & (step < n_steps))
    def _():
        last = act_ref[...]
        o_ref[...] += _dot(last, down_ref[...])
        act_ref[...] = rise()

    @pl.when(step == n_steps)
    def _():
        o_ref[...] += _dot(act_ref[...], down_ref[...])


def _mlp(x, w_up, w_down, start=None):
    rows, depth = x.shape
    hidden = w_up.shape[1]
    n_steps = 5 if hidden % 640 == 0 else 2
    blk = hidden // n_steps
    whole = pl.BlockSpec((rows, depth), lambda i: (0, 0), pipeline_mode=pl.Buffered(1))
    return pl.pallas_call(
        functools.partial(_mlp_kernel, n_steps),
        grid=(n_steps + 1,),
        in_specs=[
            whole,
            pl.BlockSpec((depth, blk), lambda i: (0, jnp.minimum(i, n_steps - 1))),
            pl.BlockSpec((blk, depth), lambda i: (jnp.maximum(i - 1, 0), 0)),
        ]
        + ([] if start is None else [whole]),
        out_specs=pl.BlockSpec((rows, depth), lambda i: (0, 0)),
        out_shape=jax.ShapeDtypeStruct((rows, depth), F32),
        scratch_shapes=[pltpu.VMEM((rows, blk), BF16)],
        cost_estimate=pl.CostEstimate(
            flops=4 * rows * depth * hidden,
            bytes_accessed=4 * depth * hidden + 6 * rows * depth,
            transcendentals=rows * hidden,
        ),
    )(x, w_up, w_down, *(() if start is None else (start,)))


def solution(mesh):
    n_seq = mesh.shape["sp"]
    n_tp = mesh.shape["tp"]
    to_right = [(sender, sender + 1) for sender in range(n_seq - 1)]
    to_left = [(sender + 1, sender) for sender in range(n_seq - 1)]
    to_next = [(sender, (sender + 1) % n_tp) for sender in range(n_tp)]
    to_prev = [(sender, (sender - 1) % n_tp) for sender in range(n_tp)]
    to_twin = [(sender, (sender + n_tp // 2) % n_tp) for sender in range(n_tp)]
    assert n_tp == 4

    def layer(tokens, glob_pos, rel_bias, w_query, w_key, w_value, w_query_glob, w_out, w_up, w_down):
        local_rows, model_dim = tokens.shape
        n_heads, rel_width = rel_bias.shape
        window = (rel_width - 1) // 2
        width = w_query.shape[1]
        hd = width // n_heads
        n_glob = glob_pos.shape[0]
        glob_blk = n_glob // n_seq
        seq_len = local_rows * n_seq
        scale = hd ** -0.5
        sp_index = lax.axis_index("sp")
        tp_index = lax.axis_index("tp")
        row_start = (sp_index * local_rows).astype(jnp.int32)

        def piece(shard):
            part = shard.shape[0] // n_seq
            return lax.dynamic_slice_in_dim(shard, sp_index * part, part, 0)

        out_full = lax.all_gather(piece(w_out), ("tp", "sp"), axis=0, tiled=True)
        up_piece = lax.ppermute(piece(w_up), "tp", to_twin)
        down_piece = lax.ppermute(piece(w_down), "tp", to_twin)
        up_twin = lax.all_gather(up_piece, "sp", axis=0, tiled=True)
        down_twin = lax.all_gather(down_piece, "sp", axis=0, tiled=True)

        slot = glob_pos - row_start
        pick = (slot[:, None] == jnp.arange(local_rows, dtype=jnp.int32)[None, :]).astype(BF16)
        share = model_dim // n_tp
        glob_rows = _dot(pick, lax.dynamic_slice_in_dim(tokens, tp_index * share, share, 1)).astype(BF16)
        glob_rows = lax.all_to_all(glob_rows, "sp", 0, 0, tiled=True)

        k, v = _project(tokens, w_key, w_value)
        (q,) = _project(tokens, w_query)
        k_left = lax.ppermute(k[local_rows - window:], "sp", to_right)
        v_left = lax.ppermute(v[local_rows - window:], "sp", to_right)
        k_right = lax.ppermute(k[:window], "sp", to_left)
        v_right = lax.ppermute(v[:window], "sp", to_left)

        def to_all(block, axes, size):
            copies = jnp.broadcast_to(block[None], (size,) + block.shape)
            return lax.all_to_all(copies, axes, 0, 0, tiled=True)

        glob_rows = glob_rows.reshape(n_seq, glob_blk, share).astype(F32).sum(axis=0).astype(BF16)
        glob_rows = to_all(glob_rows, "tp", n_tp)
        glob_rows = glob_rows.transpose(1, 0, 2).reshape(glob_blk, model_dim)
        glob_qkv = jnp.concatenate([_dot(glob_rows, w).astype(BF16) for w in (w_query_glob, w_key, w_value)], axis=1)
        glob_qkv = to_all(glob_qkv, "sp", n_seq).reshape(n_glob, 3 * width)
        glob_q = glob_qkv[:, :width]
        glob_k = glob_qkv[:, width:2 * width]
        glob_v = glob_qkv[:, 2 * width:]

        parts = _glob_partial(glob_q, k, v, n_heads, scale)
        parts = lax.all_to_all(parts, "sp", 0, 0, tiled=True).reshape(n_seq, glob_blk, parts.shape[1])
        part_max = parts[:, :, width:width + n_heads]
        factor = jnp.exp2(part_max - part_max.max(axis=0))
        tot_sum = (parts[:, :, width + n_heads:width + 2 * n_heads] * factor).sum(axis=0)
        part_out = parts[:, :, :width].reshape(n_seq, glob_blk, n_heads, hd)
        tot_out = (part_out * factor[..., None]).sum(axis=0) / tot_sum[..., None]
        glob_out = to_all(tot_out.astype(BF16).reshape(glob_blk, width), ("tp", "sp"), n_tp * n_seq)
        glob_out = glob_out.reshape(n_tp, n_glob, width).transpose(1, 0, 2).reshape(n_glob, n_tp * width)

        pad = jnp.full((n_heads, 3 * window - rel_width), NEG_INF, F32)
        bias_rows = jnp.concatenate([rel_bias * LOG2E, pad], axis=1)[:, None, :]
        blk = local_rows // (2 * n_tp)
        own_tokens = lax.dynamic_index_in_dim(tokens.reshape(2, n_tp, blk, model_dim), tp_index, 1, keepdims=False)
        hidden = []
        for half, (k_halo, v_halo) in enumerate(((k_left, v_left), (k_right, v_right))):
            win_out = _local_attn(
                half, row_start, q, k, v, k_halo, v_halo, glob_k, glob_v, bias_rows, glob_pos, window, seq_len, scale
            )
            win_out = win_out.reshape(n_tp, blk, width)
            held = [lax.dynamic_index_in_dim(win_out, tp_index, 0, keepdims=False)]
            for shift in range(1, n_tp):
                sent = lax.dynamic_index_in_dim(win_out, lax.rem(tp_index + shift, n_tp), 0, keepdims=False)
                held.append(lax.ppermute(sent, "tp", [(i, (i + shift) % n_tp) for i in range(n_tp)]))
            held = jnp.stack(held)
            win_out = jnp.concatenate(
                [
                    lax.dynamic_index_in_dim(held, lax.rem(tp_index - source + n_tp, n_tp), 0, keepdims=False)
                    for source in range(n_tp)
                ],
                axis=1,
            )
            first = row_start + half * (local_rows // 2) + tp_index * blk
            put = (first + jnp.arange(blk, dtype=jnp.int32))[:, None] == glob_pos[None, :]
            attn_rows = jnp.where(
                put.any(axis=1, keepdims=True), _dot(put.astype(BF16), glob_out).astype(BF16), win_out
            )
            hidden.append((own_tokens[half].astype(F32) + _dot(attn_rows, out_full)).astype(BF16))

        there, home = (to_next, to_prev), (to_prev, to_next)
        guests = []
        for half in range(2):
            guests.append(lax.ppermute(hidden[half], "tp", there[half]))
        own_part = [_mlp(hidden[half], w_up, w_down) for half in range(2)]
        back = []
        for half in range(2):
            guest_part = _mlp(guests[half], w_up, w_down)
            guest_part = _mlp(guests[half], up_twin, down_twin, guest_part)
            back.append(lax.ppermute(guest_part, "tp", home[half]))
        outs = []
        for half in range(2):
            part = _mlp(hidden[half], up_twin, down_twin, own_part[half])
            out = (hidden[half].astype(F32) + (part + back[half])).astype(BF16)
            outs.append(lax.all_gather(out, "tp", axis=0, tiled=True))
        return jnp.concatenate(outs, axis=0)

    row_spec = P(("batch", "sp"), None)
    col_spec = P(None, "tp")
    head_spec = P("tp", None)
    in_specs = (row_spec, P("batch"), head_spec, col_spec, col_spec, col_spec, col_spec, head_spec, col_spec, head_spec)
    return jax.shard_map(layer, mesh=mesh, in_specs=in_specs, out_specs=row_spec, check_vma=False)
```

```python
import functools
import math

import jax
import jax.numpy as jnp
from jax import lax
from jax.experimental import pallas as pl
from jax.experimental.pallas import tpu as pltpu
from jax.sharding import PartitionSpec as P


LOG2E = math.log2(math.e)
NEG_INF = float("-inf")
F32 = jnp.float32
BF16 = jnp.bfloat16


def _dot(lhs, rhs):
    return jnp.dot(lhs, rhs, preferred_element_type=F32)


def _dot_t(lhs, rhs):
    return lax.dot_general(lhs, rhs, (((1,), (1,)), ((), ())), preferred_element_type=F32)


def _proj_kernel(x_ref, *refs):
    x = x_ref[...]
    n_out = len(refs) // 2
    for w_ref, o_ref in zip(refs[:n_out], refs[n_out:]):
        o_ref[...] = _dot(x, w_ref[...]).astype(BF16)


def _project(tokens, *weights):
    rows, depth = tokens.shape
    cols = weights[0].shape[1]
    n_out = len(weights)
    blk = rows // 4
    w_spec = pl.BlockSpec((depth, cols), lambda i: (0, 0), pipeline_mode=pl.Buffered(1))
    o_spec = pl.BlockSpec((blk, cols), lambda i: (i, 0))
    return pl.pallas_call(
        _proj_kernel,
        grid=(rows // blk,),
        in_specs=[pl.BlockSpec((blk, depth), lambda i: (i, 0))] + [w_spec] * n_out,
        out_specs=[o_spec] * n_out,
        out_shape=[jax.ShapeDtypeStruct((rows, cols), BF16)] * n_out,
        cost_estimate=pl.CostEstimate(
            flops=2 * n_out * rows * depth * cols,
            bytes_accessed=2 * (rows * depth + n_out * depth * cols + n_out * rows * cols),
            transcendentals=0,
        ),
    )(tokens, *weights)


def _glob_kernel(scale, n_heads, q_ref, k_ref, v_ref, o_ref):
    hd = q_ref.shape[1] // n_heads
    rows, lanes = q_ref.shape[0], o_ref.shape[1] - q_ref.shape[1]
    lane = lax.broadcasted_iota(jnp.int32, (rows, lanes), 1)
    stats = jnp.zeros((rows, lanes), F32)
    for h in range(n_heads):
        cols = slice(h * hd, (h + 1) * hd)
        scores = _dot_t(q_ref[:, cols], k_ref[:, cols]) * scale
        top = jnp.max(scores, axis=1, keepdims=True)
        probs = jnp.exp2(scores - top)
        total = jnp.sum(probs, axis=1, keepdims=True)
        o_ref[:, cols] = _dot(probs.astype(BF16), v_ref[:, cols])
        stats = jnp.where(lane == h, top, jnp.where(lane == n_heads + h, total, stats))
    o_ref[:, q_ref.shape[1]:] = stats


def _glob_partial(glob_q, keys, values, n_heads, scale):
    n_glob, width = glob_q.shape
    rows = keys.shape[0]
    blk = n_glob // 4
    out_width = width + 128
    kv_spec = pl.BlockSpec((rows, width), lambda i: (0, 0), pipeline_mode=pl.Buffered(1))
    return pl.pallas_call(
        functools.partial(_glob_kernel, scale * LOG2E, n_heads),
        grid=(n_glob // blk,),
        in_specs=[pl.BlockSpec((blk, width), lambda i: (i, 0)), kv_spec, kv_spec],
        out_specs=pl.BlockSpec((blk, out_width), lambda i: (i, 0)),
        out_shape=jax.ShapeDtypeStruct((n_glob, out_width), F32),
        cost_estimate=pl.CostEstimate(
            flops=16 * n_glob * rows * width,
            bytes_accessed=4 * rows * width + 6 * n_glob * width,
            transcendentals=n_glob * rows * n_heads,
        ),
        name="glob_attn",
    )(glob_q, keys, values)


def _local_kernel(
    half, window, seq_len, scale, n_heads, start_ref, q_ref, k_ref, v_ref, kl_ref, kr_ref, vl_ref, vr_ref,
    gk_ref, gv_ref, rb_ref, gpos_ref, o_ref, k_ext, v_ext, bias_ref,
):
    step = pl.program_id(0)
    blk = 2 * step + half
    span = 3 * window
    rows_all = k_ref.shape[0]
    hd = q_ref.shape[1] // n_heads

    @pl.when(step == 0)
    def _():
        for ext, left, mid, right in ((k_ext, kl_ref, k_ref, kr_ref), (v_ext, vl_ref, v_ref, vr_ref)):
            ext[:window] = left[...]
            ext[window:window + rows_all] = mid[...]
            ext[window + rows_all:] = right[...]
        group = 8
        row = lax.broadcasted_iota(jnp.int32, (group, span), 0)
        for h in range(n_heads):
            bias = jnp.broadcast_to(rb_ref[h], (group, span))
            for bit in range(group.bit_length() - 1):
                bias = jnp.where(((row >> bit) & 1) == 1, pltpu.roll(bias, 1 << bit, 1), bias)
            bias_ref[h, :group] = bias
            for g in range(1, window // group):
                bias_ref[h, g * group:(g + 1) * group] = pltpu.roll(bias, g * group, 1)

    first = start_ref[0] + blk * window
    key_pos = first - window + lax.broadcasted_iota(jnp.int32, (1, span), 1)
    edge = jnp.where((key_pos >= 0) & (key_pos < seq_len), 0.0, NEG_INF).astype(F32)
    dist = first + lax.broadcasted_iota(jnp.int32, (window, 1), 0) - gpos_ref[...]
    far = jnp.where(jnp.abs(dist) > window, 0.0, NEG_INF).astype(F32)
    rows = pl.ds(pl.multiple_of(blk * window, window), span)
    for h in range(n_heads):
        cols = slice(h * hd, (h + 1) * hd)
        q = q_ref[:, cols]
        win = _dot_t(q, k_ext[rows, cols]) * scale + (bias_ref[h] + edge)
        glob = _dot_t(q, gk_ref[:, cols]) * scale + far
        top = jnp.maximum(jnp.max(win, axis=1, keepdims=True), jnp.max(glob, axis=1, keepdims=True))
        win = jnp.exp2(win - top)
        glob = jnp.exp2(glob - top)
        inv = 1.0 / (jnp.sum(win, axis=1, keepdims=True) + jnp.sum(glob, axis=1, keepdims=True))
        out = _dot((win * inv).astype(BF16), v_ext[rows, cols])
        out = out + _dot((glob * inv).astype(BF16), gv_ref[:, cols])
        o_ref[:, cols] = out.astype(BF16)


def _local_attn(half, row_start, q, k, v, halos, glob_k, glob_v, bias_rows, glob_pos, window, seq_len, scale):
    rows, width = q.shape
    n_heads = bias_rows.shape[0]
    n_glob = glob_k.shape[0]
    span = 3 * window
    n_blk = rows // (2 * window)

    def whole(array):
        return pl.BlockSpec(array.shape, lambda c, s: (0,) * array.ndim, pipeline_mode=pl.Buffered(1))

    held = (k, v, *halos, glob_k, glob_v, bias_rows, glob_pos[None, :])
    grid_spec = pltpu.PrefetchScalarGridSpec(
        num_scalar_prefetch=1,
        grid=(n_blk,),
        in_specs=[pl.BlockSpec((window, width), lambda c, s: (2 * c + half, 0))] + [whole(array) for array in held],
        out_specs=pl.BlockSpec((window, width), lambda c, s: (c, 0)),
        scratch_shapes=[
            pltpu.VMEM((rows + 2 * window, width), BF16),
            pltpu.VMEM((rows + 2 * window, width), BF16),
            pltpu.VMEM((n_heads, window, span), F32),
        ],
    )
    return pl.pallas_call(
        functools.partial(_local_kernel, half, window, seq_len, scale * LOG2E, n_heads),
        grid_spec=grid_spec,
        out_shape=jax.ShapeDtypeStruct((rows // 2, width), BF16),
        cost_estimate=pl.CostEstimate(
            flops=8 * rows * (span + n_glob) * width,
            bytes_accessed=2 * (rows * width + 2 * (rows + 2 * window + n_glob) * width),
            transcendentals=n_heads * rows * (span + n_glob) // 2,
        ),
    )(row_start[None], q, *held)


def _mlp_kernel(n_steps, x_ref, up_ref, down_ref, *refs):
    o_ref, act_ref = refs[-2:]
    step = pl.program_id(0)

    def rise():
        return jax.nn.gelu(_dot(x_ref[...], up_ref[...])).astype(BF16)

    @pl.when(step == 0)
    def _():
        act_ref[...] = rise()
        o_ref[...] = refs[0][...] if len(refs) == 3 else jnp.zeros_like(o_ref)

    @pl.when((step > 0) & (step < n_steps))
    def _():
        last = act_ref[...]
        o_ref[...] += _dot(last, down_ref[...])
        act_ref[...] = rise()

    @pl.when(step == n_steps)
    def _():
        o_ref[...] += _dot(act_ref[...], down_ref[...])


def _mlp(x, w_up, w_down, start=None):
    rows, depth = x.shape
    hidden = w_up.shape[1]
    n_steps = 5 if hidden % 640 == 0 else 2
    blk = hidden // n_steps
    whole = pl.BlockSpec((rows, depth), lambda i: (0, 0), pipeline_mode=pl.Buffered(1))
    return pl.pallas_call(
        functools.partial(_mlp_kernel, n_steps),
        grid=(n_steps + 1,),
        in_specs=[
            whole,
            pl.BlockSpec((depth, blk), lambda i: (0, jnp.minimum(i, n_steps - 1))),
            pl.BlockSpec((blk, depth), lambda i: (jnp.maximum(i - 1, 0), 0)),
        ]
        + ([] if start is None else [whole]),
        out_specs=pl.BlockSpec((rows, depth), lambda i: (0, 0)),
        out_shape=jax.ShapeDtypeStruct((rows, depth), F32),
        scratch_shapes=[pltpu.VMEM((rows, blk), BF16)],
        cost_estimate=pl.CostEstimate(
            flops=4 * rows * depth * hidden,
            bytes_accessed=4 * depth * hidden + 6 * rows * depth,
            transcendentals=rows * hidden,
        ),
    )(x, w_up, w_down, *(() if start is None else (start,)))


def solution(mesh):
    n_seq = mesh.shape["sp"]
    n_tp = mesh.shape["tp"]
    to_right = [(sender, sender + 1) for sender in range(n_seq - 1)]
    to_left = [(sender + 1, sender) for sender in range(n_seq - 1)]
    to_next = [(sender, (sender + 1) % n_tp) for sender in range(n_tp)]
    to_prev = [(sender, (sender - 1) % n_tp) for sender in range(n_tp)]
    to_twin = [(sender, (sender + n_tp // 2) % n_tp) for sender in range(n_tp)]
    assert n_tp == 4

    def layer(tokens, glob_pos, rel_bias, w_query, w_key, w_value, w_query_glob, w_out, w_up, w_down):
        local_rows, model_dim = tokens.shape
        n_heads, rel_width = rel_bias.shape
        window = (rel_width - 1) // 2
        width = w_query.shape[1]
        hd = width // n_heads
        n_glob = glob_pos.shape[0]
        glob_blk = n_glob // n_seq
        seq_len = local_rows * n_seq
        scale = hd ** -0.5
        sp_index = lax.axis_index("sp")
        tp_index = lax.axis_index("tp")
        row_start = (sp_index * local_rows).astype(jnp.int32)

        def piece(shard):
            part = shard.shape[0] // n_seq
            return lax.dynamic_slice_in_dim(shard, sp_index * part, part, 0)

        out_full = lax.all_gather(piece(w_out), ("tp", "sp"), axis=0, tiled=True)
        up_piece = lax.ppermute(piece(w_up), "tp", to_twin)
        down_piece = lax.ppermute(piece(w_down), "tp", to_twin)
        up_twin = lax.all_gather(up_piece, "sp", axis=0, tiled=True)
        down_twin = lax.all_gather(down_piece, "sp", axis=0, tiled=True)

        slot = glob_pos - row_start
        pick = (slot[:, None] == jnp.arange(local_rows, dtype=jnp.int32)[None, :]).astype(BF16)
        share = model_dim // n_tp
        glob_rows = _dot(pick, lax.dynamic_slice_in_dim(tokens, tp_index * share, share, 1)).astype(BF16)
        glob_rows = lax.all_to_all(glob_rows, "sp", 0, 0, tiled=True)

        k, v = _project(tokens, w_key, w_value)
        (q,) = _project(tokens, w_query)
        halos = []
        for rows, route in ((k[local_rows - window:], to_right), (k[:window], to_left), (v[local_rows - window:], to_right), (v[:window], to_left)):
            halos.append(lax.ppermute(rows, "sp", route))

        def to_all(block, axes, size):
            copies = jnp.broadcast_to(block[None], (size,) + block.shape)
            return lax.all_to_all(copies, axes, 0, 0, tiled=True)

        glob_rows = glob_rows.reshape(n_seq, glob_blk, share).astype(F32).sum(axis=0).astype(BF16)
        glob_rows = to_all(glob_rows, "tp", n_tp)
        glob_rows = glob_rows.transpose(1, 0, 2).reshape(glob_blk, model_dim)
        glob_q = to_all(_dot(glob_rows, w_query_glob).astype(BF16), "sp", n_seq).reshape(n_glob, width)
        glob_kv = jnp.concatenate([_dot(glob_rows, w).astype(BF16) for w in (w_key, w_value)], axis=1)
        glob_kv = to_all(glob_kv, "sp", n_seq).reshape(n_glob, 2 * width)
        glob_k = glob_kv[:, :width]
        glob_v = glob_kv[:, width:]

        parts = _glob_partial(glob_q, k, v, n_heads, scale)
        parts = lax.all_to_all(parts, "sp", 0, 0, tiled=True).reshape(n_seq, glob_blk, parts.shape[1])
        part_max = parts[:, :, width:width + n_heads]
        factor = jnp.exp2(part_max - part_max.max(axis=0))
        tot_sum = (parts[:, :, width + n_heads:width + 2 * n_heads] * factor).sum(axis=0)
        part_out = parts[:, :, :width].reshape(n_seq, glob_blk, n_heads, hd)
        tot_out = (part_out * factor[..., None]).sum(axis=0) / tot_sum[..., None]
        glob_out = to_all(tot_out.astype(BF16).reshape(glob_blk, width), ("tp", "sp"), n_tp * n_seq)
        glob_out = glob_out.reshape(n_tp, n_glob, width).transpose(1, 0, 2).reshape(n_glob, n_tp * width)

        pad = jnp.full((n_heads, 3 * window - rel_width), NEG_INF, F32)
        bias_rows = jnp.concatenate([rel_bias * LOG2E, pad], axis=1)[:, None, :]
        blk = local_rows // (2 * n_tp)
        assert blk == window
        rows_held = []
        for half in range(2):
            win_out = _local_attn(
                half, row_start, q, k, v, halos, glob_k, glob_v, bias_rows, glob_pos, window, seq_len, scale
            )
            win_out = win_out.reshape(n_tp, blk, width)
            held = [lax.dynamic_index_in_dim(win_out, tp_index, 0, keepdims=False)]
            for shift in range(1, n_tp):
                sent = lax.dynamic_index_in_dim(win_out, lax.rem(tp_index + shift, n_tp), 0, keepdims=False)
                held.append(lax.ppermute(sent, "tp", [(i, (i + shift) % n_tp) for i in range(n_tp)]))
            held = jnp.stack(held)
            rows_held.append(
                jnp.concatenate(
                    [
                        lax.dynamic_index_in_dim(held, lax.rem(tp_index - source + n_tp, n_tp), 0, keepdims=False)
                        for source in range(n_tp)
                    ],
                    axis=1,
                )
            )
        rows_held = jnp.concatenate(rows_held, axis=0)
        own_first = tp_index * 2 * blk
        put = (row_start + own_first + jnp.arange(2 * blk, dtype=jnp.int32))[:, None] == glob_pos[None, :]
        attn_rows = jnp.where(put.any(axis=1, keepdims=True), _dot(put.astype(BF16), glob_out).astype(BF16), rows_held)
        own_tokens = lax.dynamic_slice_in_dim(tokens, own_first, 2 * blk, 0)
        hidden = (own_tokens.astype(F32) + _dot(attn_rows, out_full)).astype(BF16)

        guest_0 = lax.ppermute(hidden[:blk], "tp", to_next)
        guest_1 = lax.ppermute(hidden[blk:], "tp", to_prev)
        own_part = _mlp(hidden, w_up, w_down)
        guests = jnp.concatenate([guest_0, guest_1], axis=0)
        guest_part = _mlp(guests, w_up, w_down)
        guest_part = _mlp(guests, up_twin, down_twin, guest_part)
        back_0 = lax.ppermute(guest_part[:blk], "tp", to_prev)
        back_1 = lax.ppermute(guest_part[blk:], "tp", to_next)
        own_part = _mlp(hidden, up_twin, down_twin, own_part)
        part = own_part + jnp.concatenate([back_0, back_1], axis=0)
        out = (hidden.astype(F32) + part).astype(BF16)
        return lax.all_gather(out, "tp", axis=0, tiled=True)

    row_spec = P(("batch", "sp"), None)
    col_spec = P(None, "tp")
    head_spec = P("tp", None)
    in_specs = (row_spec, P("batch"), head_spec, col_spec, col_spec, col_spec, col_spec, head_spec, col_spec, head_spec)
    return jax.shard_map(layer, mesh=mesh, in_specs=in_specs, out_specs=row_spec, check_vma=False)
```

```python
import functools
import math

import jax
import jax.numpy as jnp
from jax import lax
from jax.experimental import pallas as pl
from jax.experimental.pallas import tpu as pltpu
from jax.sharding import PartitionSpec as P


LOG2E = math.log2(math.e)
NEG_INF = float("-inf")
F32 = jnp.float32
BF16 = jnp.bfloat16


def _dot(lhs, rhs):
    return jnp.dot(lhs, rhs, preferred_element_type=F32)


def _dot_t(lhs, rhs):
    return lax.dot_general(lhs, rhs, (((1,), (1,)), ((), ())), preferred_element_type=F32)


def _proj_kernel(x_ref, *refs):
    x = x_ref[...]
    n_out = len(refs) // 2
    for w_ref, o_ref in zip(refs[:n_out], refs[n_out:]):
        o_ref[...] = _dot(x, w_ref[...]).astype(BF16)


def _project(tokens, *weights):
    rows, depth = tokens.shape
    cols = weights[0].shape[1]
    n_out = len(weights)
    blk = rows // 4
    w_spec = pl.BlockSpec((depth, cols), lambda i: (0, 0), pipeline_mode=pl.Buffered(1))
    o_spec = pl.BlockSpec((blk, cols), lambda i: (i, 0))
    return pl.pallas_call(
        _proj_kernel,
        grid=(rows // blk,),
        in_specs=[pl.BlockSpec((blk, depth), lambda i: (i, 0))] + [w_spec] * n_out,
        out_specs=[o_spec] * n_out,
        out_shape=[jax.ShapeDtypeStruct((rows, cols), BF16)] * n_out,
        cost_estimate=pl.CostEstimate(
            flops=2 * n_out * rows * depth * cols,
            bytes_accessed=2 * (rows * depth + n_out * depth * cols + n_out * rows * cols),
            transcendentals=0,
        ),
    )(tokens, *weights)


def _glob_kernel(scale, n_heads, q_ref, k_ref, v_ref, o_ref):
    hd = q_ref.shape[1] // n_heads
    rows, lanes = q_ref.shape[0], o_ref.shape[1] - q_ref.shape[1]
    lane = lax.broadcasted_iota(jnp.int32, (rows, lanes), 1)
    stats = jnp.zeros((rows, lanes), F32)
    for h in range(n_heads):
        cols = slice(h * hd, (h + 1) * hd)
        scores = _dot_t(q_ref[:, cols], k_ref[:, cols]) * scale
        top = jnp.max(scores, axis=1, keepdims=True)
        probs = jnp.exp2(scores - top)
        total = jnp.sum(probs, axis=1, keepdims=True)
        o_ref[:, cols] = _dot(probs.astype(BF16), v_ref[:, cols])
        stats = jnp.where(lane == h, top, jnp.where(lane == n_heads + h, total, stats))
    o_ref[:, q_ref.shape[1]:] = stats


def _glob_partial(glob_q, keys, values, n_heads, scale):
    n_glob, width = glob_q.shape
    rows = keys.shape[0]
    blk = n_glob // 4
    out_width = width + 128
    kv_spec = pl.BlockSpec((rows, width), lambda i: (0, 0), pipeline_mode=pl.Buffered(1))
    return pl.pallas_call(
        functools.partial(_glob_kernel, scale * LOG2E, n_heads),
        grid=(n_glob // blk,),
        in_specs=[pl.BlockSpec((blk, width), lambda i: (i, 0)), kv_spec, kv_spec],
        out_specs=pl.BlockSpec((blk, out_width), lambda i: (i, 0)),
        out_shape=jax.ShapeDtypeStruct((n_glob, out_width), F32),
        cost_estimate=pl.CostEstimate(
            flops=16 * n_glob * rows * width,
            bytes_accessed=4 * rows * width + 6 * n_glob * width,
            transcendentals=n_glob * rows * n_heads,
        ),
        name="glob_attn",
    )(glob_q, keys, values)


def _local_kernel(
    half, window, seq_len, scale, n_heads, start_ref, q_ref, k_ref, v_ref, kl_ref, kr_ref, vl_ref, vr_ref,
    gk_ref, gv_ref, rb_ref, gpos_ref, o_ref, k_ext, v_ext, bias_ref,
):
    step = pl.program_id(0)
    blk = 2 * step + half
    span = 3 * window
    rows_all = k_ref.shape[0]
    hd = q_ref.shape[1] // n_heads

    @pl.when(step == 0)
    def _():
        for ext, left, mid, right in ((k_ext, kl_ref, k_ref, kr_ref), (v_ext, vl_ref, v_ref, vr_ref)):
            ext[:window] = left[...]
            ext[window:window + rows_all] = mid[...]
            ext[window + rows_all:] = right[...]
        group = 8
        row = lax.broadcasted_iota(jnp.int32, (group, span), 0)
        for h in range(n_heads):
            bias = jnp.broadcast_to(rb_ref[h], (group, span))
            for bit in range(group.bit_length() - 1):
                bias = jnp.where(((row >> bit) & 1) == 1, pltpu.roll(bias, 1 << bit, 1), bias)
            bias_ref[h, :group] = bias
            for g in range(1, window // group):
                bias_ref[h, g * group:(g + 1) * group] = pltpu.roll(bias, g * group, 1)

    first = start_ref[0] + blk * window
    key_pos = first - window + lax.broadcasted_iota(jnp.int32, (1, span), 1)
    edge = jnp.where((key_pos >= 0) & (key_pos < seq_len), 0.0, NEG_INF).astype(F32)
    dist = first + lax.broadcasted_iota(jnp.int32, (window, 1), 0) - gpos_ref[...]
    far = jnp.where(jnp.abs(dist) > window, 0.0, NEG_INF).astype(F32)
    rows = pl.ds(pl.multiple_of(blk * window, window), span)
    for h in range(n_heads):
        cols = slice(h * hd, (h + 1) * hd)
        q = q_ref[:, cols]
        win = _dot_t(q, k_ext[rows, cols]) * scale + (bias_ref[h] + edge)
        glob = _dot_t(q, gk_ref[:, cols]) * scale + far
        top = jnp.maximum(jnp.max(win, axis=1, keepdims=True), jnp.max(glob, axis=1, keepdims=True))
        win = jnp.exp2(win - top)
        glob = jnp.exp2(glob - top)
        inv = 1.0 / (jnp.sum(win, axis=1, keepdims=True) + jnp.sum(glob, axis=1, keepdims=True))
        out = _dot((win * inv).astype(BF16), v_ext[rows, cols])
        out = out + _dot((glob * inv).astype(BF16), gv_ref[:, cols])
        o_ref[:, cols] = out.astype(BF16)


def _local_attn(half, row_start, q, k, v, halos, glob_k, glob_v, bias_rows, glob_pos, window, seq_len, scale):
    rows, width = q.shape
    n_heads = bias_rows.shape[0]
    n_glob = glob_k.shape[0]
    span = 3 * window
    n_blk = rows // (2 * window)

    def whole(array):
        return pl.BlockSpec(array.shape, lambda c, s: (0,) * array.ndim, pipeline_mode=pl.Buffered(1))

    held = (k, v, *halos, glob_k, glob_v, bias_rows, glob_pos[None, :])
    grid_spec = pltpu.PrefetchScalarGridSpec(
        num_scalar_prefetch=1,
        grid=(n_blk,),
        in_specs=[pl.BlockSpec((window, width), lambda c, s: (2 * c + half, 0))] + [whole(array) for array in held],
        out_specs=pl.BlockSpec((window, width), lambda c, s: (c, 0)),
        scratch_shapes=[
            pltpu.VMEM((rows + 2 * window, width), BF16),
            pltpu.VMEM((rows + 2 * window, width), BF16),
            pltpu.VMEM((n_heads, window, span), F32),
        ],
    )
    return pl.pallas_call(
        functools.partial(_local_kernel, half, window, seq_len, scale * LOG2E, n_heads),
        grid_spec=grid_spec,
        out_shape=jax.ShapeDtypeStruct((rows // 2, width), BF16),
        cost_estimate=pl.CostEstimate(
            flops=8 * rows * (span + n_glob) * width,
            bytes_accessed=2 * (rows * width + 2 * (rows + 2 * window + n_glob) * width),
            transcendentals=n_heads * rows * (span + n_glob) // 2,
        ),
    )(row_start[None], q, *held)


def _mlp_kernel(n_steps, n_x, n_start, *refs):
    x_refs, refs = refs[:n_x], refs[n_x:]
    (up_ref, down_ref), refs = refs[:2], refs[2:]
    starts, refs = refs[:n_start], refs[n_start:]
    outs, (x_ref, act_ref) = refs[:n_x], refs[n_x:]
    step = pl.program_id(0)
    blk = x_refs[0].shape[0]

    def rise():
        return jax.nn.gelu(_dot(x_ref[...], up_ref[...])).astype(BF16)

    def fall(act):
        part = _dot(act, down_ref[...])
        for i, out in enumerate(outs):
            out[...] += part[i * blk:(i + 1) * blk]

    @pl.when(step == 0)
    def _():
        for i in range(n_x):
            x_ref[i * blk:(i + 1) * blk] = x_refs[i][...]
            outs[i][...] = starts[i][...] if starts else jnp.zeros_like(outs[i])
        act_ref[...] = rise()

    @pl.when((step > 0) & (step < n_steps))
    def _():
        last = act_ref[...]
        fall(last)
        act_ref[...] = rise()

    @pl.when(step == n_steps)
    def _():
        fall(act_ref[...])


def _mlp(blk, xs, w_up, w_down, starts=()):
    depth, hidden = w_up.shape
    n_x = len(xs)
    rows = n_x * blk
    n_steps = 5 if hidden % 640 == 0 else 2
    cut = hidden // n_steps

    def block(at):
        return pl.BlockSpec((blk, depth), lambda i: (at, 0), pipeline_mode=pl.Buffered(1))

    return pl.pallas_call(
        functools.partial(_mlp_kernel, n_steps, n_x, len(starts)),
        grid=(n_steps + 1,),
        in_specs=[block(at) for _, at in xs]
        + [
            pl.BlockSpec((depth, cut), lambda i: (0, jnp.minimum(i, n_steps - 1))),
            pl.BlockSpec((cut, depth), lambda i: (jnp.maximum(i - 1, 0), 0)),
        ]
        + [block(at) for _, at in starts],
        out_specs=[pl.BlockSpec((blk, depth), lambda i: (0, 0))] * n_x,
        out_shape=[jax.ShapeDtypeStruct((blk, depth), F32)] * n_x,
        scratch_shapes=[pltpu.VMEM((rows, depth), BF16), pltpu.VMEM((rows, cut), BF16)],
        cost_estimate=pl.CostEstimate(
            flops=4 * rows * depth * hidden,
            bytes_accessed=4 * depth * hidden + 6 * rows * depth,
            transcendentals=rows * hidden,
        ),
    )(*[x for x, _ in xs], w_up, w_down, *[x for x, _ in starts])


def _weave_kernel(first_ref, second_ref, o_ref):
    sub = first_ref.shape[0]
    o_ref[:sub] = first_ref[...]
    o_ref[sub:] = second_ref[...]


def _weave(sub, first, second):
    rows, cols = first.shape
    spec = pl.BlockSpec((sub, cols), lambda i: (i, 0))
    return pl.pallas_call(
        _weave_kernel,
        grid=(rows // sub,),
        in_specs=[spec, spec],
        out_specs=pl.BlockSpec((2 * sub, cols), lambda i: (i, 0)),
        out_shape=jax.ShapeDtypeStruct((2 * rows, cols), first.dtype),
        cost_estimate=pl.CostEstimate(flops=rows * cols, bytes_accessed=8 * rows * cols, transcendentals=0),
        name="weave",
    )(first, second)


def solution(mesh):
    n_seq = mesh.shape["sp"]
    n_tp = mesh.shape["tp"]
    to_right = [(sender, sender + 1) for sender in range(n_seq - 1)]
    to_left = [(sender + 1, sender) for sender in range(n_seq - 1)]
    to_next = [(sender, (sender + 1) % n_tp) for sender in range(n_tp)]
    to_prev = [(sender, (sender - 1) % n_tp) for sender in range(n_tp)]
    to_twin = [(sender, (sender + n_tp // 2) % n_tp) for sender in range(n_tp)]
    assert n_tp == 4

    def layer(tokens, glob_pos, rel_bias, w_query, w_key, w_value, w_query_glob, w_out, w_up, w_down):
        local_rows, model_dim = tokens.shape
        n_heads, rel_width = rel_bias.shape
        window = (rel_width - 1) // 2
        width = w_query.shape[1]
        hd = width // n_heads
        n_glob = glob_pos.shape[0]
        glob_blk = n_glob // n_seq
        seq_len = local_rows * n_seq
        scale = hd ** -0.5
        sp_index = lax.axis_index("sp")
        tp_index = lax.axis_index("tp")
        row_start = (sp_index * local_rows).astype(jnp.int32)

        def piece(shard):
            part = shard.shape[0] // n_seq
            return lax.dynamic_slice_in_dim(shard, sp_index * part, part, 0)

        out_full = lax.all_gather(piece(w_out), ("tp", "sp"), axis=0, tiled=True)
        up_piece = lax.ppermute(piece(w_up), "tp", to_twin)
        down_piece = lax.ppermute(piece(w_down), "tp", to_twin)
        up_twin = lax.all_gather(up_piece, "sp", axis=0, tiled=True)
        down_twin = lax.all_gather(down_piece, "sp", axis=0, tiled=True)

        slot = glob_pos - row_start
        pick = (slot[:, None] == jnp.arange(local_rows, dtype=jnp.int32)[None, :]).astype(BF16)
        share = model_dim // n_tp
        glob_rows = _dot(pick, lax.dynamic_slice_in_dim(tokens, tp_index * share, share, 1)).astype(BF16)
        glob_rows = lax.all_to_all(glob_rows, "sp", 0, 0, tiled=True)

        k, v = _project(tokens, w_key, w_value)
        (q,) = _project(tokens, w_query)
        halos = []
        for rows, route in ((k[local_rows - window:], to_right), (k[:window], to_left), (v[local_rows - window:], to_right), (v[:window], to_left)):
            halos.append(lax.ppermute(rows, "sp", route))

        def to_all(block, axes, size):
            copies = jnp.broadcast_to(block[None], (size,) + block.shape)
            return lax.all_to_all(copies, axes, 0, 0, tiled=True)

        glob_rows = glob_rows.reshape(n_seq, glob_blk, share).astype(F32).sum(axis=0).astype(BF16)
        glob_rows = to_all(glob_rows, "tp", n_tp)
        glob_rows = glob_rows.transpose(1, 0, 2).reshape(glob_blk, model_dim)
        glob_q = to_all(_dot(glob_rows, w_query_glob).astype(BF16), "sp", n_seq).reshape(n_glob, width)
        glob_kv = jnp.concatenate([_dot(glob_rows, w).astype(BF16) for w in (w_key, w_value)], axis=1)
        glob_kv = to_all(glob_kv, "sp", n_seq).reshape(n_glob, 2 * width)
        glob_k = glob_kv[:, :width]
        glob_v = glob_kv[:, width:]

        parts = _glob_partial(glob_q, k, v, n_heads, scale)
        parts = lax.all_to_all(parts, "sp", 0, 0, tiled=True).reshape(n_seq, glob_blk, parts.shape[1])
        part_max = parts[:, :, width:width + n_heads]
        factor = jnp.exp2(part_max - part_max.max(axis=0))
        tot_sum = (parts[:, :, width + n_heads:width + 2 * n_heads] * factor).sum(axis=0)
        part_out = parts[:, :, :width].reshape(n_seq, glob_blk, n_heads, hd)
        tot_out = (part_out * factor[..., None]).sum(axis=0) / tot_sum[..., None]
        glob_out = to_all(tot_out.astype(BF16).reshape(glob_blk, width), ("tp", "sp"), n_tp * n_seq)
        glob_out = glob_out.reshape(n_tp, n_glob, width).transpose(1, 0, 2).reshape(n_glob, n_tp * width)

        pad = jnp.full((n_heads, 3 * window - rel_width), NEG_INF, F32)
        bias_rows = jnp.concatenate([rel_bias * LOG2E, pad], axis=1)[:, None, :]
        blk = local_rows // (2 * n_tp)
        assert blk == window
        rows_held = []
        for half in range(2):
            win_out = _local_attn(
                half, row_start, q, k, v, halos, glob_k, glob_v, bias_rows, glob_pos, window, seq_len, scale
            )
            win_out = win_out.reshape(n_tp, blk, width)
            held = [lax.dynamic_index_in_dim(win_out, tp_index, 0, keepdims=False)]
            for shift in range(1, n_tp):
                sent = lax.dynamic_index_in_dim(win_out, lax.rem(tp_index + shift, n_tp), 0, keepdims=False)
                held.append(lax.ppermute(sent, "tp", [(i, (i + shift) % n_tp) for i in range(n_tp)]))
            held = jnp.stack(held)
            rows_held.append(
                jnp.concatenate(
                    [
                        lax.dynamic_index_in_dim(held, lax.rem(tp_index - source + n_tp, n_tp), 0, keepdims=False)
                        for source in range(n_tp)
                    ],
                    axis=1,
                )
            )
        rows_held = jnp.concatenate(rows_held, axis=0)
        own_first = tp_index * 2 * blk
        put = (row_start + own_first + jnp.arange(2 * blk, dtype=jnp.int32))[:, None] == glob_pos[None, :]
        attn_rows = jnp.where(put.any(axis=1, keepdims=True), _dot(put.astype(BF16), glob_out).astype(BF16), rows_held)
        own_tokens = lax.dynamic_slice_in_dim(tokens, own_first, 2 * blk, 0)
        hidden = (own_tokens.astype(F32) + _dot(attn_rows, out_full)).astype(BF16)

        guest_0 = lax.ppermute(hidden[:blk], "tp", to_next)
        guest_1 = lax.ppermute(hidden[blk:], "tp", to_prev)
        (own_part,) = _mlp(2 * blk, [(hidden, 0)], w_up, w_down)
        guests = (guest_0, guest_1)
        guest_part = _mlp(blk, [(guest, 0) for guest in guests], w_up, w_down)

        sub = blk // 2
        back = []
        for turn in range(2):
            parts = _mlp(
                sub, [(guest, turn) for guest in guests], up_twin, down_twin,
                [(part, turn) for part in guest_part],
            )
            for part, route in zip(parts, (to_prev, to_next)):
                back.append(lax.ppermute(part, "tp", route))
        outs = []
        for turn in range(2):
            parts = _mlp(
                sub, [(hidden, turn), (hidden, 2 + turn)], up_twin, down_twin,
                [(own_part, turn), (own_part, 2 + turn)],
            )
            out = [
                (hidden[(2 * side + turn) * sub:(2 * side + turn + 1) * sub].astype(F32) + (parts[side] + back[2 * turn + side])).astype(BF16)
                for side in range(2)
            ]
            out = jnp.concatenate(out, axis=0)
            if turn == 0:
                out, own_part = lax.optimization_barrier((out, own_part))
            outs.append(lax.all_gather(out, "tp", axis=0, tiled=True))
        return _weave(sub, *outs)

    row_spec = P(("batch", "sp"), None)
    col_spec = P(None, "tp")
    head_spec = P("tp", None)
    in_specs = (row_spec, P("batch"), head_spec, col_spec, col_spec, col_spec, col_spec, head_spec, col_spec, head_spec)
    return jax.shard_map(layer, mesh=mesh, in_specs=in_specs, out_specs=row_spec, check_vma=False)
```
